32 devices in a mesh: dep: 4 (over z), col: 2 (over y), row: 4 (over x, core).
Axes of the slice: x: 2, y: 2, z: 4, core: 2. Of those that a mesh axis runs over, the one named last changes fastest.
Arguments:
- a_mat: bfloat16 [5120, 5120], P('row', 'col')
- b_mat: bfloat16 [5120, 5120], P('row', 'col')
Outputs:
- output: float32 [5120, 5120], P('row', ('col', 'dep'))
All inputs are finite; a program needn't handle non-finite values.
Results may differ from the reference program's by a relative error of at most 0.001.
Values are sent between devices in bfloat16 or wider.
A program may use at most 1 GiB of HBM per device.

```python
import jax
import jax.numpy as jnp

N = 5120


def setup_inputs(seed: int = 0) -> dict:
    key = jax.random.key(seed)
    key_a, key_b = jax.random.split(key)
    a_mat = (jax.random.normal(key_a, (N, N), jnp.float32) * N ** -0.5).astype(jnp.bfloat16)
    b_mat = jax.random.normal(key_b, (N, N), jnp.float32).astype(jnp.bfloat16)
    return {"a_mat": a_mat, "b_mat": b_mat}


def reference(a_mat, b_mat):
    return jnp.dot(a_mat, b_mat, preferred_element_type=jnp.float32)
```

```python
import functools

import jax
import jax.numpy as jnp
from jax import lax
from jax.experimental import pallas as pl
from jax.experimental.pallas import tpu as pltpu
from jax.sharding import PartitionSpec as P

MESH = pl.DeviceIdType.MESH

NY = 16
N_A = 8
N_E = 6
NK = 10
NB = 5
K_A = 5
K_P = 7
N_P = 18
K_R = 11
LAG = 2


def kernel(a_ref, b_ref, o_ref, am, bm, pm, ys, yr, zs, zr, as_, ar, bs, br, es, er, ps, pr, xs, xr, ds_, dr, fs, fr, ls, lr, loc):
    z, y, row = lax.axis_index("dep"), lax.axis_index("col"), lax.axis_index("row")
    x, c = row // 2, row % 2
    rows, depth = a_ref.shape
    quarter = b_ref.shape[0]
    width = o_ref.shape[1]
    ch = rows // 40
    blk = 4 * ch
    kc = quarter // NK
    side = z // 2
    mid = (z == 1) | (z == 2)
    end = jnp.logical_not(mid)
    eq = x == y
    neq = jnp.logical_not(eq)
    mine = (8 + 16 * side) * ch
    oth = (24 - 16 * side) * ch
    end_slice = 3 * side
    to_y = (z, 1 - y, row)
    to_x = (z, y, (1 - x) * 2 + c)
    to_core = (z, y, x * 2 + 1 - c)
    to_pair = (z + 1 - 2 * (z % 2), y, row)
    to_mid = (3 - z, y, row)

    def span(start, n):
        return pl.ds(pl.multiple_of(start, n), n)

    def within(i, n):
        return jnp.clip(i, 0, n - 1)

    def remote(src, dst, send, recv, dev):
        return pltpu.make_async_remote_copy(src_ref=src, dst_ref=dst, send_sem=send, recv_sem=recv, device_id=dev, device_id_type=MESH)

    def copy_y(k):
        k = within(k, NY)
        r = jnp.where(mid, mine + ch * k, jnp.where(k < N_A, ch * k, oth + ch * k))
        return remote(a_ref.at[span(r, ch)], am.at[1, span(r, ch)], ys.at[k], yr.at[k], to_y)

    def pass_rows(r, send, recv, dev):
        return remote(am.at[1, span(r, ch)], am.at[1, span(r, ch)], send, recv, dev)

    def copy_zm(k):
        k = within(k, NY)
        return pass_rows(mine + ch * k, zs.at[k], zr.at[k], to_mid)

    def copy_ze(k):
        k = within(k, N_E)
        return pass_rows(mine + ch * k, es.at[k], er.at[k], to_pair)

    def copy_za(k):
        k = within(k, N_A)
        return pass_rows(ch * k, as_.at[k], ar.at[k], to_pair)

    def lane(i):
        return span(c * quarter + kc * i, kc)

    def copy_zb(i):
        i = within(i, NB)
        return remote(bm.at[1, lane(i)], bm.at[2, lane(i)], bs.at[i], br.at[i], to_pair)

    def copy_x(i):
        i = within(i, 2 * NK - NB)
        extra = jnp.where(mid & neq, NK - NB, 0)
        early = i < extra
        piece = within(jnp.where(early, NB + i, i - extra), NK)
        cols = pl.ds(pl.multiple_of(jnp.where(early, end_slice, z) * width, 128), width)
        slot = jnp.where(early, 2, 1)
        return remote(b_ref.at[span(piece * kc, kc), cols], bm.at[slot, lane(piece)], xs.at[i], xr.at[i], to_x)

    def copy_d(i):
        i = within(i, 2 * NK - NB)
        extra = jnp.where(mid & eq, NK - NB, 0)
        early = i < extra
        piece = within(jnp.where(early, NB + i, i - extra), NK)
        ref = bm.at[jnp.where(early, 2, 1), lane(piece)]
        return remote(ref, ref, ds_.at[i], dr.at[i], to_core)

    def copy_f(i):
        i = within(i, NB)
        ref = bm.at[2, lane(i)]
        return remote(ref, ref, fs.at[i], fr.at[i], to_core)

    own_lane = span(c * quarter, quarter)

    def b_cols(s):
        return b_ref.at[:, pl.ds(pl.multiple_of(s * width, 128), width)]

    load_a = pltpu.make_async_copy(a_ref, am.at[0], loc.at[0])
    load_b = pltpu.make_async_copy(b_cols(z), bm.at[0, own_lane], loc.at[1])
    load_e = pltpu.make_async_copy(b_cols(end_slice), bm.at[2, own_lane], loc.at[2])
    give_b = remote(b_cols(z), bm.at[0, own_lane], ls.at[0], lr.at[0], to_core)
    give_e = remote(b_cols(end_slice), bm.at[2, own_lane], ls.at[1], lr.at[1], to_core)

    def sum_row(j):
        k, t = K_P + j // 2, j % 2
        first = jnp.where(k < K_P + 8, oth + ch * (k - K_P), mine + ch * (NY - 1))
        return jnp.where(t == 0, first, mine + ch * (k - 1))

    def copy_p(j):
        j = within(j, N_P)
        ref = pm.at[span(j * ch, ch)]
        return remote(ref, ref, ps.at[j], pr.at[j], to_pair)

    n_send = jnp.where(mid & neq, 2 * NK - NB, NK)
    n_recv = jnp.where(mid & eq, 2 * NK - NB, NK)

    barrier = pltpu.get_barrier_semaphore()
    for dev in (to_y, to_x, to_core, to_pair):
        pl.semaphore_signal(barrier, inc=1, device_id=dev, device_id_type=MESH)

    @pl.when(mid)
    def _():
        pl.semaphore_signal(barrier, inc=1, device_id=to_mid, device_id_type=MESH)

    pl.semaphore_wait(barrier, jnp.where(mid, 5, 4))

    @pl.loop(0, NY)
    def _(k):
        copy_y(k).start()

        @pl.when(k < n_send)
        def _():
            copy_x(k).start()

    load_b.start()
    give_b.start()
    load_a.start()

    @pl.when(mid & neq)
    def _():
        load_e.start()
        give_e.start()

    @pl.loop(0, rows // ch)
    def _(i):
        o_ref[span(i * ch, ch), :] = jnp.zeros((ch, width), jnp.float32)

    def add_product(half, start, slot, n):
        r = pl.ds(pl.multiple_of(jnp.clip(start, 0, rows - n), n if n < blk else ch), n)
        o_ref[r, :] += jnp.dot(am[half, r, :], bm[slot], preferred_element_type=jnp.float32)

    oth_slot = jnp.where(eq, 1, 0)
    own_slot = jnp.where(eq, 0, 1)

    def take_sums(j):
        j = within(j, N_P)
        copy_p(j).wait_recv()
        o_ref[span(sum_row(j), ch), :] += pm[span(j * ch, ch), :]

    @pl.loop(0, NY)
    def _(k):
        copy_y(k).wait_recv()

        @pl.when(mid)
        def _():
            copy_zm(k).start()

        @pl.when(mid & (k < N_E))
        def _():
            copy_ze(k).start()

        @pl.when(k < n_recv)
        def _():
            copy_x(k).wait_recv()
            copy_d(k).start()

        @pl.when(end & eq & (k < NB))
        def _():
            copy_zb(k).start()

        @pl.when(end & (k >= K_A) & (k < K_A + N_A))
        def _():
            copy_za(k - K_A).start()

        @pl.when(mid & eq & (k >= LAG) & (k < LAG + NB))
        def _():
            copy_zb(k - LAG).wait_recv()
            copy_f(k - LAG).start()

        @pl.when(mid & (k >= LAG))
        def _():
            copy_zm(k - LAG).wait_recv()

        @pl.when(mid & (k >= LAG + K_A) & (k < LAG + K_A + N_A))
        def _():
            copy_za(k - LAG - K_A).wait_recv()

        @pl.when(end & (k >= LAG) & (k < LAG + N_E))
        def _():
            copy_ze(k - LAG).wait_recv()

        @pl.when(k == 1)
        def _():
            load_b.wait()
            give_b.wait_recv()
            load_a.wait()

            @pl.when(mid & neq)
            def _():
                load_e.wait()
                give_e.wait_recv()

        @pl.when(mid & eq & (k == K_P))
        def _():
            @pl.loop(0, NB)
            def _(i):
                copy_d(i).wait_recv()
                copy_f(i).wait_recv()

        @pl.when(mid & (k >= K_P))
        def _():
            @pl.loop(0, 2)
            def _(t):
                j = 2 * (k - K_P) + t
                pm[span(j * ch, ch), :] = jnp.dot(am[1, span(sum_row(j), ch), :], bm[2], preferred_element_type=jnp.float32)
                copy_p(j).start()

        @pl.when((k == K_R) & (end | neq))
        def _():
            @pl.loop(0, NK)
            def _(i):
                copy_d(i).wait_recv()

        own_from = jnp.where(eq, 2, K_R)
        neq_mid_row = jnp.where(k % 4 == 0, mine + blk * (k // 4 - 1), jnp.where(k % 4 == 1, oth + blk * (k // 4 - 1), jnp.where(k == 10, 0, blk)))
        neq_mid_do = (k >= 4) & ((k % 4 < 2) | (k == 10) | (k == 14))
        neq_end_row = jnp.where(k == 4, 0, jnp.where(k == 8, blk, oth + 2 * blk))
        neq_end_do = (k == 4) | (k == 8) | (k == 12)
        eq_end_row = jnp.where(k == K_R, 0, jnp.where(k == K_R + 1, blk, oth + 2 * blk))
        eq_end_do = (k >= K_R) & (k < K_R + 3)
        late_row = jnp.where(mid, neq_mid_row, jnp.where(eq, eq_end_row, neq_end_row))
        late_do = (mid & neq & neq_mid_do) | (end & neq & neq_end_do) | (end & eq & eq_end_do)

        @pl.loop(0, 3)
        def _(t):
            own = t < 2
            do = jnp.where(own, (k >= own_from) & (k < own_from + 5), late_do)

            @pl.when(do)
            def _():
                start = jnp.where(own, blk * (2 * (k - own_from) + t), late_row)
                add_product(jnp.where(own, 0, 1), start, jnp.where(own, own_slot, oth_slot), blk)

        @pl.when(end & (k == jnp.where(eq, 14, 9)))
        def _():
            @pl.loop(0, N_E // 2)
            def _(t):
                add_product(1, mine + 2 * ch * t, oth_slot, 2 * ch)

        @pl.when(end & (k >= K_P + 3))
        def _():
            @pl.loop(0, 2)
            def _(t):
                take_sums(2 * (k - K_P - 3) + t)

    @pl.when(mid)
    def _():
        @pl.loop(NY - LAG, NY - 1)
        def _(k):
            copy_zm(k).wait_recv()

        @pl.when(eq)
        def _():
            @pl.loop(NK - NB, 2 * NK - NB)
            def _(i):
                copy_d(i).wait_recv()

    @pl.loop(0, 10)
    def _(t):
        last = t == 9
        all_row = jnp.where(t < 2, blk * t, jnp.where(t < 6, mine + blk * (t - 2), oth + blk * (t - 6)))
        start = jnp.where(last, oth + 3 * blk, jnp.where(eq, all_row, mine + 3 * blk))

        @pl.when(mid & last)
        def _():
            copy_zm(NY - 1).wait_recv()

        @pl.when(last | (mid & (eq | (t == 0))))
        def _():
            add_product(1, start, oth_slot, blk)

    @pl.when(end)
    def _():
        @pl.loop(2 * (NY - K_P - 3), N_P)
        def _(j):
            take_sums(j)

    @pl.loop(0, NY)
    def _(k):
        copy_y(k).wait_send()

        @pl.when(k < n_send)
        def _():
            copy_x(k).wait_send()

        @pl.when(k < n_recv)
        def _():
            copy_d(k).wait_send()

        @pl.when(mid)
        def _():
            copy_zm(k).wait_send()

        @pl.when(mid & (k < N_E))
        def _():
            copy_ze(k).wait_send()

        @pl.when(end & (k < N_A))
        def _():
            copy_za(k).wait_send()

        @pl.when(end & eq & (k < NB))
        def _():
            copy_zb(k).wait_send()

        @pl.when(mid & eq & (k < NB))
        def _():
            copy_f(k).wait_send()

    give_b.wait_send()

    @pl.when(mid & neq)
    def _():
        give_e.wait_send()

    @pl.when(mid)
    def _():
        @pl.loop(0, N_P)
        def _(j):
            copy_p(j).wait_send()


def solution(mesh):
    def body(a, b):
        rows, depth = a.shape
        quarter, wide = b.shape
        width = wide // mesh.shape["dep"]
        dma = pltpu.SemaphoreType.DMA
        counts = (NY, NY, NY, NY, N_A, N_A, NB, NB, N_E, N_E, N_P, N_P, NY, NY, NY, NY, NB, NB, 2, 2, 3)
        return pl.pallas_call(
            kernel,
            out_shape=jax.ShapeDtypeStruct((rows, width), jnp.float32),
            in_specs=[pl.BlockSpec(memory_space=pl.ANY)] * 2,
            out_specs=pl.BlockSpec(memory_space=pltpu.VMEM),
            scratch_shapes=[
                pltpu.VMEM((2, rows, depth), jnp.bfloat16),
                pltpu.VMEM((3, 2 * quarter, width), jnp.bfloat16),
                pltpu.VMEM((N_P * (rows // 40), width), jnp.float32),
            ]
            + [dma((n,)) for n in counts],
            compiler_params=pltpu.CompilerParams(collective_id=0, has_side_effects=True, vmem_limit_bytes=48 * 2**20),
        )(a, b)

    return jax.shard_map(body, mesh=mesh, in_specs=(P("row", "col"), P("row", "col")), out_specs=P("row", ("col", "dep")), check_vma=False)
```

```python
import jax
import jax.numpy as jnp
from jax import lax
from jax.experimental import pallas as pl
from jax.experimental.pallas import tpu as pltpu
from jax.sharding import PartitionSpec as P

MESH = pl.DeviceIdType.MESH

PIECES = 40
NY = 16
N_A = 10
N_M = 14
TOP = 30
N_E = 6
NK = 10
NB = 5
K_P = 6
N_P = 18
LAG = 2
PART = 4


def mine(p, n):
    return (p, TOP - p - n)


def oth(p, n):
    return (TOP - p - n, p)


def grp_a(p):
    return (TOP + p, TOP + p)


def own(j):
    return (4 * j, 4 * j)


def schedule(mid, eq):
    plan = {k: [] for k in range(NY + 1)}

    def put(k, kind, start, half=1):
        plan[k].append((kind, start[0] + 64 * start[1] + 4096 * half))

    first = 1 if eq else 10
    for j in range(10):
        put(first + j // 2, "big", own(j), 0)
    if mid and not eq:
        for i in range(3):
            put(4 * i + 4, "big", mine(4 * i, 4))
            put(4 * i + 5, "big", oth(4 * i, 4))
        put(6, "big", grp_a(0))
        put(10, "big", grp_a(4))
        put(12, "small", grp_a(8))
        put(15, "small", oth(12, 2))
        put(NY, "big", mine(12, 4))
    elif mid:
        order = [(9, 14, mine(0, 4)), (9, 14, oth(0, 4)), (10, 14, mine(4, 4)), (10, 14, oth(4, 4)), (11, 14, grp_a(0))]
        order += [(12, 15, mine(8, 4)), (13, 15, oth(8, 4)), (14, 15, grp_a(4))]
        for one, two, start in order:
            put(one, "part0", start)
            put(two, "part1", start)
        put(15, "small", oth(12, 2))
        put(15, "big", mine(12, 4))
        put(NY, "small", grp_a(8))
    elif not eq:
        put(3, "big", grp_a(0))
        put(7, "big", grp_a(4))
        put(9, "small", grp_a(8))
        put(6, "big", mine(0, 4))
        put(8, "small", mine(4, 2))
        put(13, "big", oth(10, 4))
        put(NY, "small", mine(14, 2))
    else:
        put(10, "big", grp_a(0))
        put(10, "big", grp_a(4))
        put(11, "small", grp_a(8))
        put(11, "big", mine(0, 4))
        put(12, "small", mine(4, 2))
        put(13, "big", oth(10, 4))
        put(NY, "small", mine(14, 2))
    return plan


def pick(key, table):
    code = jnp.int32(-1)
    for at, value in table:
        code = jnp.where(key == at, value, code)
    return code


def kernel(a_ref, b_ref, o_ref, am, bm, pm, ys, yr, zs, zr, as_, ar, bs, br, es, er, ps, pr, xs, xr, ds_, dr, fs, fr, ls, lr, loc):
    z, y, row = lax.axis_index("dep"), lax.axis_index("col"), lax.axis_index("row")
    x, c = row // 2, row % 2
    rows = a_ref.shape[0]
    quarter = b_ref.shape[0]
    width = o_ref.shape[1]
    ch = rows // PIECES
    kc = quarter // NK
    side = z // 2
    is_mid = (z == 1) | (z == 2)
    is_eq = x == y
    end_slice = 3 * side
    to_y = (z, 1 - y, row)
    to_x = (z, y, (1 - x) * 2 + c)
    to_core = (z, y, x * 2 + 1 - c)
    to_pair = (z + 1 - 2 * (z % 2), y, row)
    to_mid = (3 - z, y, row)

    def within(i, n):
        return jnp.clip(i, 0, n - 1)

    def span(start, n):
        return pl.ds(pl.multiple_of(start, n), n)

    def piece(p):
        return span(within(p, PIECES) * ch, ch)

    def mine_at(i):
        return i + side * (TOP - 1 - 2 * i)

    def oth_at(i):
        return TOP - 1 - i + side * (2 * i + 1 - TOP)

    def remote(src, dst, send, recv, dev):
        return pltpu.make_async_remote_copy(src_ref=src, dst_ref=dst, send_sem=send, recv_sem=recv, device_id=dev, device_id_type=MESH)

    def pass_rows(p, send, recv, dev):
        return remote(am.at[1, piece(p)], am.at[1, piece(p)], send, recv, dev)

    def copy_y(k, mid):
        p = mine_at(k) if mid else jnp.where(k < N_A, TOP + k, jnp.where(k < N_M, oth_at(k), mine_at(k)))
        k = within(k, NY)
        return remote(a_ref.at[piece(p)], am.at[1, piece(p)], ys.at[k], yr.at[k], to_y)

    def copy_zm(k):
        k = within(k, N_M)
        return pass_rows(mine_at(k), zs.at[k], zr.at[k], to_mid)

    def copy_ze(k):
        k = within(k, N_E)
        return pass_rows(mine_at(k), es.at[k], er.at[k], to_pair)

    def copy_za(k):
        k = within(k, N_A)
        return pass_rows(TOP + k, as_.at[k], ar.at[k], to_pair)

    def lane(i):
        return span(c * quarter + kc * i, kc)

    def copy_zb(i):
        i = within(i, NB)
        return remote(bm.at[1, lane(i)], bm.at[2, lane(i)], bs.at[i], br.at[i], to_pair)

    def b_piece(i, extra):
        early = i < extra
        return jnp.where(early, 2, 1), within(jnp.where(early, NB + i, i - extra), NK), early

    def copy_x(i, extra):
        slot, p, early = b_piece(i, extra)
        i = within(i, 2 * NK - NB)
        cols = pl.ds(pl.multiple_of(jnp.where(early, end_slice, z) * width, 128), width)
        return remote(b_ref.at[span(p * kc, kc), cols], bm.at[slot, lane(p)], xs.at[i], xr.at[i], to_x)

    def copy_d(i, extra):
        slot, p, _ = b_piece(i, extra)
        i = within(i, 2 * NK - NB)
        return remote(bm.at[slot, lane(p)], bm.at[slot, lane(p)], ds_.at[i], dr.at[i], to_core)

    def copy_f(i):
        i = within(i, NB)
        return remote(bm.at[2, lane(i)], bm.at[2, lane(i)], fs.at[i], fr.at[i], to_core)

    own_lane = span(c * quarter, quarter)

    def b_cols(s):
        return b_ref.at[:, pl.ds(pl.multiple_of(s * width, 128), width)]

    load_a = pltpu.make_async_copy(a_ref, am.at[0], loc.at[0])
    load_b = pltpu.make_async_copy(b_cols(z), bm.at[0, own_lane], loc.at[1])
    load_e = pltpu.make_async_copy(b_cols(end_slice), bm.at[2, own_lane], loc.at[2])
    give_b = remote(b_cols(z), bm.at[0, own_lane], ls.at[0], lr.at[0], to_core)
    give_e = remote(b_cols(end_slice), bm.at[2, own_lane], ls.at[1], lr.at[1], to_core)

    def sum_at(j):
        k, t = K_P + j // 2, j % 2
        last = k == K_P + 8
        from_oth = (t == 0) | last
        return jnp.where(from_oth, oth_at(jnp.where(last, 8 + t, k - K_P)), mine_at(k))

    def copy_p(j):
        j = within(j, N_P)
        ref = pm.at[span(j * ch, ch)]
        return remote(ref, ref, ps.at[j], pr.at[j], to_pair)

    barrier = pltpu.get_barrier_semaphore()
    for dev in (to_y, to_x, to_core, to_pair):
        pl.semaphore_signal(barrier, inc=1, device_id=dev, device_id_type=MESH)

    @pl.when(is_mid)
    def _():
        pl.semaphore_signal(barrier, inc=1, device_id=to_mid, device_id_type=MESH)

    load_b.start()
    load_a.start()
    pl.semaphore_wait(barrier, jnp.where(is_mid, 5, 4))

    def run(mid, eq):
        end = not mid
        sent_extra = NK - NB if mid and not eq else 0
        came_extra = NK - NB if mid and eq else 0
        n_send, n_recv = NK + sent_extra, NK + came_extra
        k_a = NB if eq else 0
        oth_slot, own_slot = (1, 0) if eq else (0, 1)
        plan = schedule(mid, eq)

        @pl.loop(0, NY)
        def _(k):
            copy_y(k, mid).start()

            @pl.when(k < n_send)
            def _():
                copy_x(k, sent_extra).start()

        give_b.start()
        if mid and not eq:
            load_e.start()
            give_e.start()

        @pl.loop(0, PIECES)
        def _(i):
            o_ref[span(i * ch, ch), :] = jnp.zeros((ch, width), jnp.float32)

        def multiply(kind, code):
            n = (2 if kind == "small" else 4) * ch
            half = code // 4096
            start = jnp.where(side == 0, code % 64, code // 64 % 64) * ch
            r = pl.ds(pl.multiple_of(jnp.clip(start, 0, rows - n), ch), n)
            if kind in ("big", "small"):
                slot = jnp.where(half == 1, oth_slot, own_slot)
                o_ref[r, :] += jnp.dot(am[half, r, :], bm[slot], preferred_element_type=jnp.float32)
                return
            lo, hi = (0, PART * kc) if kind == "part0" else (PART * kc, quarter)
            o_ref[r, :] += sum(
                jnp.dot(am[1, r, lo + q : hi + q], bm[1, lo + q : hi + q, :], preferred_element_type=jnp.float32)
                for q in (0, quarter)
            )

        def products(k, steps):
            for kind in ("big", "small", "part0", "part1"):
                by_step = {s: [v for name, v in plan[s] if name == kind] for s in steps}
                most = max(len(v) for v in by_step.values())
                if most == 0:
                    continue

                @pl.loop(0, most)
                def _(t):
                    code = pick(k * 8 + t, [(s * 8 + i, v) for s, vs in by_step.items() for i, v in enumerate(vs)])

                    @pl.when(code >= 0)
                    def _():
                        multiply(kind, code)

        def take_sums(j):
            j = within(j, N_P)
            copy_p(j).wait_recv()
            o_ref[piece(sum_at(j)), :] += pm[span(j * ch, ch), :]

        @pl.loop(0, NY)
        def _(k):
            copy_y(k, mid).wait_recv()

            if mid:

                @pl.when(k < N_M)
                def _():
                    copy_zm(k).start()

                @pl.when(k < N_E)
                def _():
                    copy_ze(k).start()

            @pl.when(k < n_recv)
            def _():
                copy_x(k, came_extra).wait_recv()
                copy_d(k, came_extra).start()

            if end:
                if eq:

                    @pl.when(k < NB)
                    def _():
                        copy_zb(k).start()

                @pl.when((k >= k_a) & (k < k_a + N_A))
                def _():
                    copy_za(k - k_a).start()

                @pl.when((k >= LAG) & (k < LAG + N_E))
                def _():
                    copy_ze(k - LAG).wait_recv()

            if mid:
                if eq:

                    @pl.when((k >= LAG) & (k < LAG + NB))
                    def _():
                        copy_zb(k - LAG).wait_recv()
                        copy_f(k - LAG).start()

                @pl.when((k >= LAG) & (k < LAG + N_M))
                def _():
                    copy_zm(k - LAG).wait_recv()

                @pl.when((k >= LAG + k_a) & (k < LAG + k_a + N_A))
                def _():
                    copy_za(k - LAG - k_a).wait_recv()

            @pl.when(k == 1)
            def _():
                load_b.wait()
                give_b.wait_recv()
                load_a.wait()
                if mid and not eq:
                    load_e.wait()
                    give_e.wait_recv()

            if mid:
                if eq:

                    @pl.when(k == K_P)
                    def _():
                        @pl.loop(0, NB)
                        def _(i):
                            copy_d(i, came_extra).wait_recv()
                            copy_f(i).wait_recv()

                @pl.when((k >= K_P) & (k < K_P + 9))
                def _():
                    @pl.loop(0, 2)
                    def _(t):
                        j = within(2 * (k - K_P) + t, N_P)
                        pm[span(j * ch, ch), :] = jnp.dot(am[1, piece(sum_at(j)), :], bm[2], preferred_element_type=jnp.float32)
                        copy_p(j).start()

            def b_ready(at, first, last):
                @pl.when(k == at)
                def _():
                    @pl.loop(first, last)
                    def _(i):
                        copy_d(i, came_extra).wait_recv()

            if mid and eq:
                b_ready(9, NB, NB + PART)
                b_ready(14, NB + PART, n_recv)
            else:
                b_ready(10, 0, NK)

            products(k, range(NY))

            if end:

                @pl.when(k >= K_P + 3)
                def _():
                    @pl.loop(0, 2)
                    def _(t):
                        take_sums(2 * (k - K_P - 3) + t)

        if mid and eq:

            @pl.loop(NY - LAG - k_a, N_A)
            def _(k):
                copy_za(k).wait_recv()

        products(jnp.int32(NY), [NY])

        if end:

            @pl.loop(2 * (NY - K_P - 3), N_P)
            def _(j):
                take_sums(j)

        @pl.loop(0, NY)
        def _(k):
            copy_y(k, mid).wait_send()

            @pl.when(k < n_send)
            def _():
                copy_x(k, sent_extra).wait_send()

            @pl.when(k < n_recv)
            def _():
                copy_d(k, came_extra).wait_send()

            if mid:

                @pl.when(k < N_M)
                def _():
                    copy_zm(k).wait_send()

                @pl.when(k < N_E)
                def _():
                    copy_ze(k).wait_send()

                if eq:

                    @pl.when(k < NB)
                    def _():
                        copy_f(k).wait_send()

            else:

                @pl.when(k < N_A)
                def _():
                    copy_za(k).wait_send()

                if eq:

                    @pl.when(k < NB)
                    def _():
                        copy_zb(k).wait_send()

        give_b.wait_send()
        if mid:
            if not eq:
                give_e.wait_send()

            @pl.loop(0, N_P)
            def _(j):
                copy_p(j).wait_send()

    for mid in (True, False):
        for eq in (True, False):

            @pl.when((is_mid == mid) & (is_eq == eq))
            def _():
                run(mid, eq)


def solution(mesh):
    def body(a, b):
        rows, depth = a.shape
        quarter, wide = b.shape
        width = wide // mesh.shape["dep"]
        dma = pltpu.SemaphoreType.DMA
        counts = (NY, NY, N_M, N_M, N_A, N_A, NB, NB, N_E, N_E, N_P, N_P, NY, NY, NY, NY, NB, NB, 2, 2, 3)
        return pl.pallas_call(
            kernel,
            out_shape=jax.ShapeDtypeStruct((rows, width), jnp.float32),
            in_specs=[pl.BlockSpec(memory_space=pl.ANY)] * 2,
            out_specs=pl.BlockSpec(memory_space=pltpu.VMEM),
            scratch_shapes=[
                pltpu.VMEM((2, rows, depth), jnp.bfloat16),
                pltpu.VMEM((3, 2 * quarter, width), jnp.bfloat16),
                pltpu.VMEM((N_P * (rows // PIECES), width), jnp.float32),
            ]
            + [dma((n,)) for n in counts],
            compiler_params=pltpu.CompilerParams(collective_id=0, has_side_effects=True, vmem_limit_bytes=48 * 2**20),
        )(a, b)

    return jax.shard_map(body, mesh=mesh, in_specs=(P("row", "col"), P("row", "col")), out_specs=P("row", ("col", "dep")), check_vma=False)
```

```python
import jax
import jax.numpy as jnp
from jax import lax
from jax.experimental import pallas as pl
from jax.experimental.pallas import tpu as pltpu
from jax.sharding import PartitionSpec as P

MESH = pl.DeviceIdType.MESH

PIECES = 40
NY = 16
N_A = 10
N_M = 14
TOP = 30
N_E = 5
NK = 10
NB = 4
N_X = NK - NB
K_P = 5
N_P = 19
LAG = 2
PART = 6
ROWS = {"big": 4, "small": 2, "tiny": 1, "part0": 4, "part1": 8, "part1w": 12}


def mine(p, n):
    return (p, TOP - p - n)


def oth(p, n):
    return (TOP - p - n, p)


def grp_a(p):
    return (TOP + p, TOP + p)


def own(j):
    return (4 * j, 4 * j)


def schedule(mid, eq):
    plan = {k: [] for k in range(NY + 1)}

    def put(k, kind, start, half=1):
        plan[k].append((kind, start[0] + 64 * start[1] + 4096 * half))

    first = 1 if eq else 10
    for j in range(10):
        put(first + j // 2, "big", own(j), 0)
    if mid and not eq:
        for i in range(3):
            put(4 * i + 4, "big", mine(4 * i, 4))
            put(4 * i + 5, "big", oth(4 * i, 4))
        put(6, "big", grp_a(0))
        put(9, "big", grp_a(4))
        put(15, "small", grp_a(8))
    elif mid:
        order = [(12, mine(0, 4)), (12, oth(0, 4)), (12, grp_a(0)), (13, mine(4, 4)), (13, oth(4, 4)), (13, mine(8, 4))]
        order += [(14, oth(8, 4)), (14, grp_a(4))]
        for k, start in order:
            put(k, "part0", start)
        put(14, "part1w", mine(0, 12))
        put(14, "part1w", oth(0, 12))
        put(14, "part1", grp_a(0))
    else:
        late = eq
        put(10 if late else 3, "big", grp_a(0))
        put(10 if late else 7, "big", grp_a(4))
        put(11 if late else 9, "small", grp_a(8))
        put(11 if late else 6, "big", mine(0, 4))
        put(12 if late else 8, "tiny", mine(4, 1))
        put(13, "big", oth(10, 4))
        put(NY, "small", mine(14, 2))
    return plan


def pick(key, table):
    code = jnp.int32(-1)
    for at, value in table:
        code = jnp.where(key == at, value, code)
    return code


def kernel(a_ref, b_ref, o_ref, am, bm, pm, yr, gr, hr, br, xr, dr, lr, sent):
    z, y, row = lax.axis_index("dep"), lax.axis_index("col"), lax.axis_index("row")
    x, c = row // 2, row % 2
    rows = a_ref.shape[0]
    quarter = b_ref.shape[0]
    width = o_ref.shape[1]
    ch = rows // PIECES
    kc = quarter // NK
    side = z // 2
    is_mid = (z == 1) | (z == 2)
    is_eq = x == y
    pair = z + 1 - 2 * (z % 2)
    to_y = (z, 1 - y, row)
    to_x = (z, y, (1 - x) * 2 + c)
    to_core = (z, y, x * 2 + 1 - c)
    to_pair = (pair, y, row)
    to_mid = (3 - z, y, row)

    def within(i, n):
        return jnp.clip(i, 0, n - 1)

    def span(start, n):
        return pl.ds(pl.multiple_of(start, n), n)

    def piece(p):
        return span(within(p, PIECES) * ch, ch)

    def mine_at(i):
        return i + side * (TOP - 1 - 2 * i)

    def oth_at(i):
        return TOP - 1 - i + side * (2 * i + 1 - TOP)

    def remote(src, dst, send, recv, dev):
        return pltpu.make_async_remote_copy(src_ref=src, dst_ref=dst, send_sem=send, recv_sem=recv, device_id=dev, device_id_type=MESH)

    def pass_rows(p, flow, recv, dev):
        return remote(am.at[1, piece(p)], am.at[1, piece(p)], sent.at[flow], recv, dev)

    def copy_y(k, mid):
        p = mine_at(k) if mid else jnp.where(k < N_A, TOP + k, jnp.where(k < N_M, oth_at(k), mine_at(k)))
        return remote(a_ref.at[piece(p)], am.at[1, piece(p)], sent.at[0], yr.at[within(k, NY)], to_y)

    def copy_zm(k):
        k = within(k, N_M)
        return pass_rows(mine_at(k), 1, gr.at[k], to_mid)

    def copy_ze(k):
        k = within(k, N_E)
        return pass_rows(mine_at(k), 2, hr.at[k], to_pair)

    def copy_za(k):
        k = within(k, N_A)
        return pass_rows(TOP + k, 1, hr.at[k], to_pair)

    def lane(i, n=1, core=c):
        return pl.ds(pl.multiple_of(core * quarter + kc * i, kc), n * kc)

    def copy_zb(i):
        i = within(i, NB)
        return remote(bm.at[1, lane(i)], bm.at[2, lane(i)], sent.at[2], br.at[i], to_pair)

    copy_zc = remote(bm.at[2, lane(NK - 1)], bm.at[1, lane(NK - 1)], sent.at[2], br.at[NB], to_pair)

    def b_piece(i, mid, special):
        if not special:
            return 1, within(i, NK), z
        extra = (i < N_X) if mid else (i == NK)
        other = within(NB + i, NK) if mid else NK - 1
        plain = within(i - N_X if mid else i, NK)
        return jnp.where(extra, 2, 1), jnp.where(extra, other, plain), jnp.where(extra, pair, z)

    def copy_x(i, mid, special):
        slot, p, s = b_piece(i, mid, special)
        cols = pl.ds(pl.multiple_of(s * width, 128), width)
        rows_b = pl.ds(pl.multiple_of(p * kc, kc), kc)
        return remote(b_ref.at[rows_b, cols], bm.at[slot, lane(p)], sent.at[3], xr.at[within(i, NY)], to_x)

    def copy_d(slot, p, group):
        return remote(bm.at[slot, lane(p)], bm.at[slot, lane(p)], sent.at[4], dr.at[group], to_core)

    def came_d(slot, p, n, group):
        ref = bm.at[slot, lane(p, n, 1 - c)]
        remote(ref, ref, sent.at[4], dr.at[group], to_core).wait_recv()

    def all_sent(flow, ref):
        remote(ref, ref, sent.at[flow], lr.at[0], to_core).wait_send()

    own_lane = span(c * quarter, quarter)

    def b_cols(s):
        return b_ref.at[:, pl.ds(pl.multiple_of(s * width, 128), width)]

    load_a = pltpu.make_async_copy(a_ref, am.at[0], lr.at[2])
    load_b = pltpu.make_async_copy(b_cols(z), bm.at[0, own_lane], lr.at[3])
    load_e = pltpu.make_async_copy(b_cols(pair), bm.at[2, own_lane], lr.at[4])
    give_b = remote(b_cols(z), bm.at[0, own_lane], sent.at[5], lr.at[0], to_core)
    give_e = remote(b_cols(pair), bm.at[2, own_lane], sent.at[6], lr.at[1], to_core)

    def sum_at(j):
        k = K_P + j // 2
        return jnp.where(j % 2 == 0, oth_at(k - K_P), mine_at(k))

    def copy_p(j):
        j = within(j, N_P)
        ref = pm.at[span(j * ch, ch)]
        return remote(ref, ref, sent.at[7], gr.at[j // 2], to_pair)

    def came_p(j, n):
        ref = pm.at[pl.ds(pl.multiple_of(within(j, N_P - n + 1) * ch, ch), n * ch)]
        remote(ref, ref, sent.at[7], gr.at[within(j // 2, (N_P + 1) // 2)], to_pair).wait_recv()

    barrier = pltpu.get_barrier_semaphore()
    for dev in (to_y, to_x, to_core, to_pair):
        pl.semaphore_signal(barrier, inc=1, device_id=dev, device_id_type=MESH)

    @pl.when(is_mid)
    def _():
        pl.semaphore_signal(barrier, inc=1, device_id=to_mid, device_id_type=MESH)

    load_b.start()
    load_a.start()
    pl.semaphore_wait(barrier, jnp.where(is_mid, 5, 4))

    def run(mid, eq):
        end = not mid
        extra = N_X - 1 if mid else 1
        n_send, n_recv = (NK, NK + extra) if eq else (NK + extra, NK)
        k_a, wait_a = (NB, NB + LAG + 1) if eq else (0, LAG)
        oth_slot, own_slot = (1, 0) if eq else (0, 1)
        plan = schedule(mid, eq)

        @pl.loop(0, NY)
        def _(k):
            copy_y(k, mid).start()

            @pl.when(k < n_send)
            def _():
                copy_x(k, mid, not eq).start()

        give_b.start()
        if mid and not eq:
            load_e.start()
            give_e.start()

        @pl.loop(0, PIECES)
        def _(i):
            o_ref[span(i * ch, ch), :] = jnp.zeros((ch, width), jnp.float32)

        def multiply(kind, code):
            n = ROWS[kind] * ch
            half = code // 4096
            start = jnp.where(side == 0, code % 64, code // 64 % 64) * ch
            r = pl.ds(pl.multiple_of(jnp.clip(start, 0, rows - n), ch), n)
            if kind in ("big", "small", "tiny"):
                slot = jnp.where(half == 1, oth_slot, own_slot)
                o_ref[r, :] += jnp.dot(am[half, r, :], bm[slot], preferred_element_type=jnp.float32)
                return
            lo, hi = (0, PART * kc) if kind == "part0" else (PART * kc, quarter)
            o_ref[r, :] += sum(
                jnp.dot(am[1, r, lo + q : hi + q], bm[1, lo + q : hi + q, :], preferred_element_type=jnp.float32)
                for q in (0, quarter)
            )

        def products(k, steps):
            for kind in ROWS:
                by_step = {s: [v for name, v in plan[s] if name == kind] for s in steps}
                most = max(len(v) for v in by_step.values())
                if most == 0:
                    continue

                @pl.loop(0, most)
                def _(t):
                    code = pick(k * 8 + t, [(s * 8 + i, v) for s, vs in by_step.items() for i, v in enumerate(vs)])

                    @pl.when(code >= 0)
                    def _():
                        multiply(kind, code)

        def take_sums(j):
            j = within(j, N_P)
            o_ref[piece(sum_at(j)), :] += pm[span(j * ch, ch), :]

        @pl.loop(0, NY)
        def _(k):
            copy_y(k, mid).wait_recv()

            if mid:

                @pl.when(k < N_M)
                def _():
                    copy_zm(k).start()

                @pl.when(k < N_E)
                def _():
                    copy_ze(k).start()

            @pl.when(k < n_recv)
            def _():
                copy_x(k, mid, eq).wait_recv()

            @pl.when(k < (NK if end else n_recv))
            def _():
                slot, p, _ = b_piece(k, mid, eq and mid)
                group = 0
                if mid and eq:
                    group = jnp.where(k < N_X, 0, jnp.where(k < N_X + PART, 1, 2))
                copy_d(slot, p, group).start()

            if end:
                if eq:

                    @pl.when(k < NB)
                    def _():
                        copy_zb(k).start()

                    @pl.when(k == NK)
                    def _():
                        copy_zc.start()

                @pl.when((k >= k_a) & (k < k_a + N_A))
                def _():
                    copy_za(k - k_a).start()

                @pl.when((k >= LAG) & (k < LAG + N_E))
                def _():
                    copy_ze(k - LAG).wait_recv()

            if mid:
                if eq:

                    @pl.when((k >= LAG) & (k < LAG + NB))
                    def _():
                        copy_zb(k - LAG).wait_recv()
                        copy_d(2, within(k - LAG, NB), 3).start()

                    @pl.when(k == 13)
                    def _():
                        copy_zc.wait_recv()
                        copy_d(1, NK - 1, 2).start()

                @pl.when((k >= LAG) & (k < LAG + N_M))
                def _():
                    copy_zm(k - LAG).wait_recv()

                @pl.when((k >= wait_a) & (k < wait_a + N_A))
                def _():
                    copy_za(k - wait_a).wait_recv()

            @pl.when(k == 1)
            def _():
                load_b.wait()
                give_b.wait_recv()
                load_a.wait()
                if mid and not eq:
                    load_e.wait()
                    give_e.wait_recv()

            if mid:
                if eq:

                    @pl.when(k == K_P)
                    def _():
                        came_d(2, NB, N_X, 0)
                        came_d(2, 0, NB, 3)

                @pl.when((k >= K_P) & (k < K_P + (N_P + 1) // 2))
                def _():
                    @pl.loop(2 * (k - K_P), jnp.minimum(2 * (k - K_P) + 2, N_P))
                    def _(j):
                        pm[span(j * ch, ch), :] = jnp.dot(am[1, piece(sum_at(j)), :], bm[2], preferred_element_type=jnp.float32)
                        copy_p(j).start()

            if mid and eq:

                @pl.when(k == 12)
                def _():
                    came_d(1, 0, PART, 1)

                @pl.when(k == 14)
                def _():
                    came_d(1, PART, NK - PART, 2)

            else:

                @pl.when(k == 10)
                def _():
                    came_d(1, 0, NK, 0)

            products(k, range(NY))

            if end:

                @pl.when(k >= K_P + 3)
                def _():
                    came_p(2 * (k - K_P - 3), 2)

                    @pl.loop(0, 2)
                    def _(t):
                        take_sums(2 * (k - K_P - 3) + t)

        if mid and eq:

            @pl.loop(NY - wait_a, N_A)
            def _(k):
                copy_za(k).wait_recv()

        if mid:
            last = [(mine(12, 4), 4), (oth(12, 2), 2)] + ([(grp_a(8), 2)] if eq else [])
            spans = [pl.ds(pl.multiple_of((s0 + side * (s1 - s0)) * ch, ch), n * ch) for (s0, s1), n in last]
            left = jnp.concatenate([am[1, r, :] for r in spans], axis=0)
            total = jnp.dot(left, bm[oth_slot], preferred_element_type=jnp.float32)
            at = 0
            for r, (_, n) in zip(spans, last):
                o_ref[r, :] += total[at : at + n * ch]
                at += n * ch
        else:
            products(jnp.int32(NY), [NY])

            @pl.loop(2 * (NY - K_P - 3), N_P, step=2)
            def _(j):
                @pl.when(j < N_P - 1)
                def _():
                    came_p(j, 2)
                    take_sums(j)
                    take_sums(j + 1)

            came_p(N_P - 1, 1)
            take_sums(N_P - 1)

        all_sent(0, am.at[0, pl.ds(0, NY * ch)])
        all_sent(1, am.at[0, pl.ds(0, (N_M if mid else N_A) * ch)])
        if mid:
            all_sent(2, am.at[0, pl.ds(0, N_E * ch)])
            all_sent(7, pm)
        elif eq:
            all_sent(2, bm.at[0, pl.ds(0, (NB + 1) * kc)])
        all_sent(3, bm.at[0, pl.ds(0, n_send * kc)])
        all_sent(4, bm.at[0, pl.ds(0, (2 * NK if mid and eq else NK) * kc)])
        all_sent(5, bm.at[0, pl.ds(0, quarter)])
        if mid and not eq:
            all_sent(6, bm.at[0, pl.ds(0, quarter)])

    for mid in (True, False):
        for eq in (True, False):

            @pl.when((is_mid == mid) & (is_eq == eq))
            def _():
                run(mid, eq)


def solution(mesh):
    def body(a, b):
        rows, depth = a.shape
        quarter, wide = b.shape
        width = wide // mesh.shape["dep"]
        dma = pltpu.SemaphoreType.DMA
        counts = (NY, N_M, N_A, NB + 1, NY, 4, 5, 8)
        return pl.pallas_call(
            kernel,
            out_shape=jax.ShapeDtypeStruct((rows, width), jnp.float32),
            in_specs=[pl.BlockSpec(memory_space=pl.ANY)] * 2,
            out_specs=pl.BlockSpec(memory_space=pltpu.VMEM),
            scratch_shapes=[
                pltpu.VMEM((2, rows, depth), jnp.bfloat16),
                pltpu.VMEM((3, 2 * quarter, width), jnp.bfloat16),
                pltpu.VMEM((N_P * (rows // PIECES), width), jnp.float32),
            ]
            + [dma((n,)) for n in counts],
            compiler_params=pltpu.CompilerParams(collective_id=0, has_side_effects=True, vmem_limit_bytes=48 * 2**20),
        )(a, b)

    return jax.shard_map(body, mesh=mesh, in_specs=(P("row", "col"), P("row", "col")), out_specs=P("row", ("col", "dep")), check_vma=False)
```

```python
import jax
import jax.numpy as jnp
from jax import lax
from jax.experimental import pallas as pl
from jax.experimental.pallas import tpu as pltpu
from jax.sharding import PartitionSpec as P

MESH = pl.DeviceIdType.MESH

PIECES = 40
NY = 16
N_A = 10
N_M = 14
TOP = 30
N_E = 5
NK = 10
NB = 4
N_X = NK - NB
K_P = 5
N_P = 19
LAG = 2
PARTS = (0, 6, 8, NK)
KINDS = {
    "big": (4, None),
    "small": (2, None),
    "tiny": (1, None),
    "first4": (4, 0),
    "first12": (12, 0),
    "next8": (8, 1),
    "next12": (12, 1),
    "rest8": (8, 2),
    "rest12": (12, 2),
}


def mine(p, n):
    return (p, TOP - p - n)


def oth(p, n):
    return (TOP - p - n, p)


def grp_a(p):
    return (TOP + p, TOP + p)


def own(j):
    return (4 * j, 4 * j)


def schedule(mid, eq):
    plan = {k: [] for k in range(NY + 1)}

    def put(k, kind, start, half=1, late=0, only=False):
        plan[k].append((kind, start[0] + 64 * start[1] + 4096 * half, late, only))

    first = 1 if eq else 10
    for j in range(10):
        put(first + j // 2, "big", own(j), 0)
    if mid and not eq:
        for i in range(3):
            put(4 * i + 4, "big", mine(4 * i, 4))
            put(4 * i + 5, "big", oth(4 * i, 4), late=1)
        put(6, "big", grp_a(0))
        put(9, "big", grp_a(4))
        put(15, "small", grp_a(8))
    elif mid:
        put(12, "first12", mine(0, 12))
        put(12, "first4", grp_a(0))
        put(13, "first12", oth(0, 12), late=1)
        put(14, "first4", grp_a(4))
        for part in ("next", "rest"):
            put(14, part + "12", mine(0, 12))
            put(14, part + "12", oth(0, 12))
            put(14, part + "8", grp_a(0))
    else:
        late = eq
        put(10 if late else 3, "big", grp_a(0))
        put(10 if late else 7, "big", grp_a(4))
        put(11 if late else 9, "small", grp_a(8))
        put(11 if late else 6, "big", mine(0, 4))
        put(12 if late else 8, "tiny", mine(4, 1))
        put(12 if late else 8, "tiny", mine(5, 1), only=True)
        put(13, "big", oth(10, 4))
        put(NY, "small", mine(14, 2))
    return plan


def pick(key, table):
    code = jnp.int32(-1)
    for at, value in table:
        code = jnp.where(key == at, value, code)
    return code


def kernel(a_ref, b_ref, o_ref, am, bm, pm, yr, gr, hr, br, xr, dr, lr, sent):
    z, y, row = lax.axis_index("dep"), lax.axis_index("col"), lax.axis_index("row")
    x, c = row // 2, row % 2
    rows = a_ref.shape[0]
    quarter = b_ref.shape[0]
    width = o_ref.shape[1]
    ch = rows // PIECES
    kc = quarter // NK
    side = z // 2
    is_mid = (z == 1) | (z == 2)
    is_eq = x == y
    pair = z + 1 - 2 * (z % 2)
    n_e, n_p, k_p = N_E + c, N_P - c, K_P + c
    to_y = (z, 1 - y, row)
    to_x = (z, y, (1 - x) * 2 + c)
    to_core = (z, y, x * 2 + 1 - c)
    to_pair = (pair, y, row)
    to_mid = (3 - z, y, row)

    def within(i, n):
        return jnp.clip(i, 0, n - 1)

    def span(start, n):
        return pl.ds(pl.multiple_of(start, n), n)

    def piece(p):
        return span(within(p, PIECES) * ch, ch)

    def mine_at(i):
        return i + side * (TOP - 1 - 2 * i)

    def oth_at(i):
        return TOP - 1 - i + side * (2 * i + 1 - TOP)

    def remote(src, dst, send, recv, dev):
        return pltpu.make_async_remote_copy(src_ref=src, dst_ref=dst, send_sem=send, recv_sem=recv, device_id=dev, device_id_type=MESH)

    def pass_rows(p, flow, recv, dev):
        return remote(am.at[1, piece(p)], am.at[1, piece(p)], sent.at[flow], recv, dev)

    def copy_y(k, mid):
        p = mine_at(k) if mid else jnp.where(k < N_A, TOP + k, jnp.where(k < N_M, oth_at(k), mine_at(k)))
        return remote(a_ref.at[piece(p)], am.at[1, piece(p)], sent.at[0], yr.at[within(k, NY)], to_y)

    def copy_zm(k):
        k = within(k, N_M)
        return pass_rows(mine_at(k), 1, gr.at[k], to_mid)

    def copy_ze(k):
        k = within(k, N_E + 1)
        return pass_rows(mine_at(k), 2, hr.at[k], to_pair)

    def copy_za(k):
        k = within(k, N_A)
        return pass_rows(TOP + k, 1, hr.at[k], to_pair)

    def lane(i, n=1, core=c):
        return pl.ds(pl.multiple_of(core * quarter + kc * i, kc), n * kc)

    def copy_zb(i):
        i = within(i, NB)
        return remote(bm.at[1, lane(i)], bm.at[2, lane(i)], sent.at[2], br.at[i], to_pair)

    copy_zc = remote(bm.at[2, lane(NK - 1)], bm.at[1, lane(NK - 1)], sent.at[2], br.at[NB], to_pair)

    def b_piece(i, mid, special):
        if not special:
            return 1, within(i, NK), z
        extra = (i < N_X) if mid else (i == NK)
        other = within(NB + i, NK) if mid else NK - 1
        plain = within(i - N_X if mid else i, NK)
        return jnp.where(extra, 2, 1), jnp.where(extra, other, plain), jnp.where(extra, pair, z)

    def copy_x(i, mid, special):
        slot, p, s = b_piece(i, mid, special)
        cols = pl.ds(pl.multiple_of(s * width, 128), width)
        rows_b = pl.ds(pl.multiple_of(p * kc, kc), kc)
        return remote(b_ref.at[rows_b, cols], bm.at[slot, lane(p)], sent.at[3], xr.at[within(i, NY)], to_x)

    def copy_d(slot, p, group):
        return remote(bm.at[slot, lane(p)], bm.at[slot, lane(p)], sent.at[4], dr.at[group], to_core)

    def came_d(slot, p, n, group):
        ref = bm.at[slot, lane(p, n, 1 - c)]
        remote(ref, ref, sent.at[4], dr.at[group], to_core).wait_recv()

    def all_sent(flow, ref):
        remote(ref, ref, sent.at[flow], lr.at[0], to_core).wait_send()

    own_lane = span(c * quarter, quarter)

    def b_cols(s):
        return b_ref.at[:, pl.ds(pl.multiple_of(s * width, 128), width)]

    load_a = pltpu.make_async_copy(a_ref, am.at[0], lr.at[2])
    load_b = pltpu.make_async_copy(b_cols(z), bm.at[0, own_lane], lr.at[3])
    load_e = pltpu.make_async_copy(b_cols(pair), bm.at[2, own_lane], lr.at[4])
    give_b = remote(b_cols(z), bm.at[0, own_lane], sent.at[5], lr.at[0], to_core)
    give_e = remote(b_cols(pair), bm.at[2, own_lane], sent.at[6], lr.at[1], to_core)

    def sum_at(j):
        k = j // 2 + k_p - 1
        return jnp.where(j < 3, oth_at(j), jnp.where(j == 3, mine_at(k_p), jnp.where(j % 2 == 0, mine_at(k), oth_at(k - 3 - c))))

    def copy_p(j):
        j = within(j, N_P)
        ref = pm.at[span(j * ch, ch)]
        return remote(ref, ref, sent.at[7], gr.at[j // 2], to_pair)

    def came_p(j, n):
        ref = pm.at[pl.ds(pl.multiple_of(within(j, N_P - n + 1) * ch, ch), n * ch)]
        remote(ref, ref, sent.at[7], gr.at[within(j // 2, (N_P + 1) // 2)], to_pair).wait_recv()

    barrier = pltpu.get_barrier_semaphore()
    for dev in (to_y, to_x, to_core, to_pair):
        pl.semaphore_signal(barrier, inc=1, device_id=dev, device_id_type=MESH)

    @pl.when(is_mid)
    def _():
        pl.semaphore_signal(barrier, inc=1, device_id=to_mid, device_id_type=MESH)

    load_b.start()
    load_a.start()
    pl.semaphore_wait(barrier, jnp.where(is_mid, 5, 4))

    def run(mid, eq):
        end = not mid
        extra = N_X - 1 if mid else 1
        n_send, n_recv = (NK, NK + extra) if eq else (NK + extra, NK)
        k_a, wait_a = (NB, NB + LAG + 1) if eq else (0, LAG)
        oth_slot, own_slot = (1, 0) if eq else (0, 1)
        plan = schedule(mid, eq)

        @pl.loop(0, NY)
        def _(k):
            copy_y(k, mid).start()

            @pl.when(k < n_send)
            def _():
                copy_x(k, mid, not eq).start()

        give_b.start()
        if mid and not eq:
            load_e.start()
            give_e.start()

        @pl.loop(0, PIECES)
        def _(i):
            o_ref[span(i * ch, ch), :] = jnp.zeros((ch, width), jnp.float32)

        def multiply(kind, code):
            n, part = KINDS[kind]
            n = n * ch
            half = code // 4096
            start = jnp.where(side == 0, code % 64, code // 64 % 64) * ch
            r = pl.ds(pl.multiple_of(jnp.clip(start, 0, rows - n), ch), n)
            if part is None:
                slot = jnp.where(half == 1, oth_slot, own_slot)
                o_ref[r, :] += jnp.dot(am[half, r, :], bm[slot], preferred_element_type=jnp.float32)
                return
            lo, hi = PARTS[part] * kc, PARTS[part + 1] * kc
            o_ref[r, :] += sum(
                jnp.dot(am[1, r, lo + q : hi + q], bm[1, lo + q : hi + q, :], preferred_element_type=jnp.float32)
                for q in (0, quarter)
            )

        def products(k, steps):
            for kind in KINDS:
                if mid and eq and kind in ("next8", "rest8"):
                    part = KINDS[kind][1]

                    @pl.when(k == 14)
                    def _():
                        came_d(1, PARTS[part], PARTS[part + 1] - PARTS[part], 1 + part)

                table, most = {}, 0
                for core in (0, 1):
                    for step in steps:
                        found = [e for s in plan for e in plan[s] if e[0] == kind and s + core * e[2] == step and core >= e[3]]
                        most = max(most, len(found))
                        for i, e in enumerate(found):
                            table.setdefault(e, [-1, -1])[core] = step * 8 + i
                if most == 0:
                    continue

                @pl.loop(0, most)
                def _(t):
                    code = pick(k * 8 + t, [(jnp.where(c == 1, one, zero), e[1]) for e, (zero, one) in table.items()])

                    @pl.when(code >= 0)
                    def _():
                        multiply(kind, code)

        def take_sums(j):
            j = within(j, N_P)
            o_ref[piece(sum_at(j)), :] += pm[span(j * ch, ch), :]

        @pl.loop(0, NY)
        def _(k):
            copy_y(k, mid).wait_recv()

            if mid:

                @pl.when(k < N_M)
                def _():
                    copy_zm(k).start()

                @pl.when(k < n_e)
                def _():
                    copy_ze(k).start()

            @pl.when(k < n_recv)
            def _():
                copy_x(k, mid, eq).wait_recv()

            @pl.when(k < (NK if end else n_recv))
            def _():
                slot, p, _ = b_piece(k, mid, eq and mid)
                group = 0
                if mid and eq:
                    group = jnp.where(k < N_X, 0, jnp.where(k < N_X + PARTS[1], 1, jnp.where(k < N_X + PARTS[2], 2, 3)))
                copy_d(slot, p, group).start()

            if end:
                if eq:

                    @pl.when(k < NB)
                    def _():
                        copy_zb(k).start()

                    @pl.when(k == NK)
                    def _():
                        copy_zc.start()

                @pl.when((k >= k_a) & (k < k_a + N_A))
                def _():
                    copy_za(k - k_a).start()

                @pl.when((k >= LAG) & (k < LAG + n_e))
                def _():
                    copy_ze(k - LAG).wait_recv()

            if mid:
                if eq:

                    @pl.when((k >= LAG) & (k < LAG + NB))
                    def _():
                        copy_zb(k - LAG).wait_recv()
                        copy_d(2, within(k - LAG, NB), 4).start()

                    @pl.when(k == 13)
                    def _():
                        copy_zc.wait_recv()
                        copy_d(1, NK - 1, 3).start()

            @pl.when(k == 1)
            def _():
                load_b.wait()
                give_b.wait_recv()
                load_a.wait()
                if mid and not eq:
                    load_e.wait()
                    give_e.wait_recv()

            if mid:
                if eq:

                    @pl.when(k == k_p)
                    def _():
                        came_d(2, NB, N_X, 0)
                        came_d(2, 0, NB, 4)

                @pl.when((k >= k_p) & (k < k_p + N_P // 2))
                def _():
                    j0 = jnp.where(k == k_p, 0, 2 * (k - k_p) + 2)

                    @pl.loop(j0, jnp.minimum(2 * (k - k_p) + 4, n_p))
                    def _(j):
                        pm[span(j * ch, ch), :] = jnp.dot(am[1, piece(sum_at(j)), :], bm[2], preferred_element_type=jnp.float32)
                        copy_p(j).start()

            if mid:

                @pl.when((k >= LAG + c) & (k < LAG + c + N_M))
                def _():
                    copy_zm(k - LAG - c).wait_recv()

                @pl.when((k >= wait_a) & (k < wait_a + N_A))
                def _():
                    copy_za(k - wait_a).wait_recv()

            if mid and eq:

                @pl.when(k == 12)
                def _():
                    came_d(1, 0, PARTS[1], 1)

            else:

                @pl.when(k == 10)
                def _():
                    came_d(1, 0, NK, 0)

            products(k, range(NY))

            if end:

                @pl.when(k >= K_P + 3)
                def _():
                    came_p(2 * (k - K_P - 3), 2)

                    @pl.loop(0, 2)
                    def _(t):
                        take_sums(2 * (k - K_P - 3) + t)

        if mid and eq:

            @pl.loop(NY - wait_a, N_A)
            def _(k):
                copy_za(k).wait_recv()

        if mid:

            @pl.when(c == 1)
            def _():
                copy_zm(N_M - 1).wait_recv()

            last = [(mine(12, 4), 4), (oth(12, 2), 2)] + ([(grp_a(8), 2)] if eq else [])
            spans = [pl.ds(pl.multiple_of((s0 + side * (s1 - s0)) * ch, ch), n * ch) for (s0, s1), n in last]
            left = jnp.concatenate([am[1, r, :] for r in spans], axis=0)
            total = jnp.dot(left, bm[oth_slot], preferred_element_type=jnp.float32)
            at = 0
            for r, (_, n) in zip(spans, last):
                o_ref[r, :] += total[at : at + n * ch]
                at += n * ch
        else:
            products(jnp.int32(NY), [NY])

            @pl.loop(2 * (NY - K_P - 3), N_P, step=2)
            def _(j):
                @pl.when(j < N_P - 1)
                def _():
                    came_p(j, 2)
                    take_sums(j)
                    take_sums(j + 1)

            @pl.when(c == 0)
            def _():
                came_p(N_P - 1, 1)
                take_sums(N_P - 1)


        all_sent(0, am.at[0, pl.ds(0, NY * ch)])
        all_sent(1, am.at[0, pl.ds(0, (N_M if mid else N_A) * ch)])
        if mid:

            @pl.when(c == 0)
            def _():
                all_sent(2, am.at[0, pl.ds(0, N_E * ch)])
                all_sent(7, pm)

            @pl.when(c == 1)
            def _():
                all_sent(2, am.at[0, pl.ds(0, (N_E + 1) * ch)])
                all_sent(7, pm.at[pl.ds(0, (N_P - 1) * ch)])

        elif eq:
            all_sent(2, bm.at[0, pl.ds(0, (NB + 1) * kc)])
        all_sent(3, bm.at[0, pl.ds(0, n_send * kc)])
        all_sent(4, bm.at[0, pl.ds(0, (2 * NK if mid and eq else NK) * kc)])
        all_sent(5, bm.at[0, pl.ds(0, quarter)])
        if mid and not eq:
            all_sent(6, bm.at[0, pl.ds(0, quarter)])

    for mid in (True, False):
        for eq in (True, False):

            @pl.when((is_mid == mid) & (is_eq == eq))
            def _():
                run(mid, eq)


def solution(mesh):
    def body(a, b):
        rows, depth = a.shape
        quarter, wide = b.shape
        width = wide // mesh.shape["dep"]
        dma = pltpu.SemaphoreType.DMA
        counts = (NY, N_M, N_A, NB + 1, NY, 5, 5, 8)
        return pl.pallas_call(
            kernel,
            out_shape=jax.ShapeDtypeStruct((rows, width), jnp.float32),
            in_specs=[pl.BlockSpec(memory_space=pl.ANY)] * 2,
            out_specs=pl.BlockSpec(memory_space=pltpu.VMEM),
            scratch_shapes=[
                pltpu.VMEM((2, rows, depth), jnp.bfloat16),
                pltpu.VMEM((3, 2 * quarter, width), jnp.bfloat16),
                pltpu.VMEM((N_P * (rows // PIECES), width), jnp.float32),
            ]
            + [dma((n,)) for n in counts],
            compiler_params=pltpu.CompilerParams(collective_id=0, has_side_effects=True, vmem_limit_bytes=48 * 2**20),
        )(a, b)

    return jax.shard_map(body, mesh=mesh, in_specs=(P("row", "col"), P("row", "col")), out_specs=P("row", ("col", "dep")), check_vma=False)
```
